32 devices in a mesh: cuts: 4 (over z), row: 8 (over y, x, core).
Axes of the slice: x: 2, y: 2, z: 4, core: 2. Of those that a mesh axis runs over, the one named last changes fastest.
Arguments:
- eigvecs: float32 [16384, 2048], P('row', 'cuts'), may hold values from -1.2 to 1.2
- slice_counts: int32 [4], P('cuts'), may hold values from 256 to 512, as said below
- occ_index: int32 [2048], P('cuts'), may hold values from 0 to 63
- occ_levels: float32 [64], replicated, may hold values from 0 to 1
Outputs:
- slab: float32 [4096, 16384], P('cuts', 'row')
The draws below stay inside these ranges and needn't reach their ends.
Inputs may be any that keep to these rules, and one draw needn't show every extreme that they name: `slice_counts`: some slice holds exactly 512 eigenvalues in every draw; the others at least half of that.
All inputs are finite; a program needn't handle non-finite values.
Results may differ from the reference program's by a relative error of at most 0.000062.
Values sent between devices are 32-bit elements; how exact they have to be, the bound alone decides.
A program may use at most 128 MiB of HBM per device.

```python
import jax
import jax.numpy as jnp
from jax import lax

ORDER = 16384
BLOCK = 1024
SLAB_SUB = 256
EIG_DEV = 512
LEVELS = 64
EIGS = 2048
SLAB = 4096
N_CUTS = 4


def draw_slice_counts(key, part):
    first, second = jax.random.split(jax.random.fold_in(key, 11))
    counted = jax.random.randint(first, (N_CUTS,), EIG_DEV // 2, EIG_DEV + 1)
    full_one = jax.random.randint(second, (), 0, N_CUTS)
    return jnp.where(jnp.arange(N_CUTS) == full_one, EIG_DEV, counted).astype(jnp.int32)


def with_ends(array, stream_key, low, top_value):
    longest = array.shape.index(max(array.shape))
    spots = []
    for shift in (0, 1):
        where = [jax.random.randint(jax.random.fold_in(stream_key, axis), (), 0, length) for axis, length in enumerate(array.shape)]
        where[longest] = (where[longest] + shift) % array.shape[longest]
        spots.append(tuple(where))
    return array.at[spots[0]].set(low).at[spots[1]].set(top_value)


def block_levels(key, dims, pieces, low, largest):
    factor_of, own = 1.0, jax.random.fold_in(key, 6)
    for position, shards_of in pieces:
        draws = jnp.exp(jax.random.uniform(jax.random.fold_in(own, position), (shards_of,), jnp.float32, low / len(pieces), largest / len(pieces)))
        factor_of = factor_of * jnp.repeat(draws, dims[position] // shards_of).reshape([-1 if axis == position else 1 for axis in range(len(dims))])
    return factor_of


def gaussian(own_key, shape, width, reach, pieces=(), held_as=jnp.bfloat16):
    array = jax.random.normal(own_key, shape, jnp.float32) * width
    if len(pieces) > 0:
        array = block_levels(own_key, shape, pieces, -0.22, 0.18) * array
    return jnp.clip(array, min=-reach, max=reach).astype(held_as)


def setup_inputs(seed: int = 0) -> dict:
    key_of = jax.random.split(jax.random.key(seed), 5)
    eigvecs = gaussian(key_of[0], (ORDER, EIGS), 0.18, 1.2, ((0, 8), (1, 4)), jnp.float32)
    slice_counts = draw_slice_counts(jax.random.fold_in(key_of[4], 71), 0)
    occ_index = with_ends(jax.random.randint(key_of[2], (EIGS,), 0, LEVELS), jax.random.fold_in(key_of[2], 1), 0, LEVELS - 1).astype(jnp.int32)
    occ_levels = jnp.clip(jax.random.uniform(key_of[3], (LEVELS,), jnp.float32, 0.0, 1.0), 0.0, 1.0)
    return dict(eigvecs=eigvecs, slice_counts=slice_counts, occ_index=occ_index, occ_levels=occ_levels)


def reference(eigvecs, slice_counts, occ_index, occ_levels):
    slots = jnp.arange(EIGS, dtype=jnp.int32)
    group = slots // EIG_DEV
    inside = slots - group * EIG_DEV
    live = inside < slice_counts[group]
    weights = jnp.where(live, occ_levels[occ_index], jnp.float32(0.0))
    blocks = eigvecs.reshape(ORDER // BLOCK, BLOCK, EIGS)[:, :SLAB_SUB, :]
    picked = blocks.reshape(SLAB, EIGS) * weights[None, :]
    return lax.dot_general(picked, eigvecs, (((1,), (1,)), ((), ())), precision=lax.Precision.HIGHEST, preferred_element_type=jnp.float32)
```

```python
import jax
import jax.numpy as jnp
from jax import lax
from jax.experimental.layout import Layout, with_layout_constraint
from jax.sharding import PartitionSpec as P


BLOCK = 1024
SLAB_SUB = 256
SLAB = 4096
FACTOR_CHUNKS = 1


def slot_weights(slot_count, slice_counts, occ_index, occ_levels):
    level_ids = jnp.arange(occ_levels.shape[0], dtype=jnp.int32)
    one_hot = (occ_index[:, None] == level_ids[None, :]).astype(jnp.float32)
    values = jnp.dot(one_hot, occ_levels, precision=lax.Precision.HIGHEST)
    live = jnp.arange(slot_count, dtype=jnp.int32) < slice_counts[0]
    return jnp.where(live, values, jnp.float32(0.0))


def product(panel, columns):
    made = lax.dot_general(
        panel,
        columns,
        (((1,), (1,)), ((), ())),
        precision=lax.Precision.HIGH,
        preferred_element_type=jnp.float32,
    )
    return with_layout_constraint(made, Layout(major_to_minor=(0, 1)))


def shards(eigvecs, slice_counts, occ_index, occ_levels):
    row_count = eigvecs.shape[0]
    slot_count = eigvecs.shape[1]
    weights = slot_weights(slot_count, slice_counts, occ_index, occ_levels)
    local_blocks = eigvecs.reshape(row_count // BLOCK, BLOCK, slot_count)[:, :SLAB_SUB, :]
    local_rows = local_blocks.reshape(-1, slot_count) * weights[None, :]
    cut_count = lax.axis_size("cuts")
    row_devices = lax.axis_size("row")
    owned = SLAB // cut_count
    strip = slot_count // row_devices
    spread = lax.all_to_all(local_rows.T, "row", split_axis=0, concat_axis=1, tiled=True)
    owners = lax.all_to_all(spread, "cuts", split_axis=1, concat_axis=0, tiled=True)
    panels = lax.all_gather(owners, "row", axis=0, tiled=True)
    panel = (
        panels.reshape(row_devices, cut_count, strip, owned)
        .transpose(1, 0, 2, 3)
        .reshape(cut_count * slot_count, owned)
    )
    return lax.dot_general(
        panel,
        lax.all_gather(eigvecs, "cuts", axis=1, tiled=True),
        (((0,), (1,)), ((), ())),
        precision=lax.Precision.HIGH,
        preferred_element_type=jnp.float32,
    )


def line_shards(eigvecs, slice_counts, occ_index, occ_levels):
    row_count, slot_count = eigvecs.shape
    weights = slot_weights(slot_count, slice_counts, occ_index, occ_levels)
    cut = lax.axis_index("cuts")
    row = lax.axis_index("row")
    y, x, core = row // 4, (row // 2) % 2, row % 2
    inner = jnp.logical_or(cut == 1, cut == 2)

    inward = [(0, 1), (3, 2)]
    swap = [(1, 2), (2, 1)]
    outward = [(1, 0), (2, 3)]

    def along(value, pairs, axis="cuts"):
        return lax.ppermute(value, axis, pairs)

    half_y = [(8 * z + 4 * (z // 2) + k, 8 * z + 4 * (1 - z // 2) + k) for z in range(4) for k in range(4)]
    swap_x = [(r, r ^ 2) for r in range(8)]
    swap_core = [(r, r ^ 1) for r in range(8)]

    picks = row_count // BLOCK
    pieces = BLOCK // SLAB_SUB
    tail = jnp.broadcast_to(weights[None, :], (8, slot_count))
    picked = jnp.concatenate([eigvecs[b * BLOCK : b * BLOCK + SLAB_SUB] for b in range(picks)] + [tail])
    places = [(b, q) for q in range(1, pieces) for b in range(picks)]
    chunks = [eigvecs[b * BLOCK + q * SLAB_SUB : b * BLOCK + (q + 1) * SLAB_SUB] for b, q in places]

    def gather_factor(own):
        near = along(own, inward)
        other = along(own, swap)
        far = along(near, swap)
        out_own = along(own, outward)
        out_other = along(other, outward)
        out_far = along(far, outward)
        return [
            own,
            jnp.where(inner, near, out_own),
            jnp.where(inner, other, out_other),
            jnp.where(inner, far, out_far),
        ]

    def spread(value):
        rows = value[:-8] * value[-8:-7]
        got = along(rows, half_y, ("cuts", "row"))
        mine = jnp.where(y == cut // 2, rows, got)
        across = along(mine, swap_x, "row")
        here = x == cut % 2
        both = jnp.stack([jnp.where(here, mine, across), jnp.where(here, across, mine)])
        peer = along(both, swap_core, "row")
        first = jnp.where(core == 0, both, peer)
        second = jnp.where(core == 0, peer, both)
        full = jnp.concatenate([first, second], axis=1)
        return full[0], full[1]

    parts = gather_factor(picked)
    factors = [gather_factor(chunk) for chunk in chunks[:FACTOR_CHUNKS]]
    panels = [spread(part) for part in parts]
    mine = jnp.concatenate([p[0] for p in panels], axis=1)
    theirs = jnp.concatenate([panels[k][1] for k in (0, 2, 3)], axis=1)

    out = {}
    late = []
    for k in range(FACTOR_CHUNKS, len(chunks)):
        (b, q), own = places[k], chunks[k]
        near = along(own, inward)
        other = along(own, swap)
        far = along(near, swap)
        partial = product(theirs, jnp.concatenate([own, other, far], axis=1))
        late.append((b, q, own, near, other, far, along(partial, outward)))
    head = product(mine, jnp.concatenate([p[:-8] for p in parts], axis=1))
    for b in range(picks):
        out[b, 0] = head[:, b * SLAB_SUB : (b + 1) * SLAB_SUB]
    for (b, q), factor in zip(places, factors):
        out[b, q] = product(mine, jnp.concatenate(factor, axis=1))
    for b, q, own, near, other, far, sent in late:
        own_part = product(mine, jnp.concatenate([own, near, other, far], axis=1))
        out[b, q] = lax.optimization_barrier(own_part) + sent
    return jnp.concatenate([out[b, q] for b in range(picks) for q in range(pieces)], axis=1)


def solution(mesh):
    on_line = mesh.shape["cuts"] == 4 and mesh.shape["row"] == 8
    specs = dict(
        mesh=mesh,
        in_specs=(P("row", "cuts"), P("cuts"), P("cuts"), P()),
        out_specs=P("cuts", "row"),
        check_vma=False,
    )
    if not on_line:
        return jax.shard_map(shards, **specs)

    return jax.shard_map(line_shards, **specs)
```
